32 devices in a mesh: grp: 2 (over x), gy: 4 (over z), gz: 4 (over y, core).
Axes of the slice: x: 2, y: 2, z: 4, core: 2. Of those that a mesh axis runs over, the one named last changes fastest.
Arguments:
- vorticity: float32 [2, 3, 256, 256, 256], P('grp', None, 'gz', 'gy'), may hold values from -6 to 6
- wind: float32 [2, 3], P('grp'), may hold values from 0.5 to 1.2
Outputs:
- new_vorticity: float32 [2, 3, 256, 256, 256], P('grp', None, 'gz', 'gy')
- velocity: float32 [2, 3, 256, 256, 256], P('grp', None, 'gz', 'gy')
The draws below stay inside these ranges and needn't reach their ends.
All inputs are finite; a program needn't handle non-finite values.
Results may differ from the reference program's by a relative error of at most 0.0003.
Values sent between devices are 32-bit elements; how exact they have to be, the bound alone decides.
A program may use at most 192 MiB of HBM per device.

```python
import math
import jax
import jax.numpy as jnp

NX = 256
NY = 256
NZ = 256


def draw_vorticity(key, part):
    shape = (2, 3, NZ, NY, NX)
    first = jax.random.fold_in(key, 0)
    return jnp.clip(jax.random.normal(first, shape, jnp.float32), -6.0, 6.0)


def shard_levels(key, shape, cuts, smallest, largest):
    def one(position, parts):
        steps = jax.random.uniform(jax.random.fold_in(jax.random.fold_in(key, 6), position), (parts,), jnp.float32, smallest / len(cuts), largest / len(cuts))
        return jnp.repeat(jnp.exp(steps), shape[position] // parts).reshape((-1,) + (1,) * (len(shape) - position - 1))

    gain = one(*cuts[0])
    for cut in cuts[1:]:
        gain = gain * one(*cut)
    return gain


def setup_inputs(seed: int = 0) -> dict:
    key_of = jax.random.split(jax.random.key(seed), 3)
    vorticity = draw_vorticity(jax.random.fold_in(key_of[2], 71), 0)
    wind = jnp.clip(0.5 + 0.70000005 * jax.random.uniform(key_of[1], (2, 3), jnp.float32) ** shard_levels(key_of[1], (2, 3), ((0, 2),), -0.2, 0.2), 0.5, 1.2)
    return dict(vorticity=vorticity, wind=wind)


TIME_STEP = 0.4


def kernel_weight(offset):
    mag = jnp.abs(offset)
    inner = 1.0 - 2.5 * mag * mag + 1.5 * mag * mag * mag
    outer = 0.5 * (2.0 - mag) * (2.0 - mag) * (1.0 - mag)
    return jnp.where(mag < 1.0, inner, jnp.where(mag < 2.0, outer, 0.0 * mag))


def wave_numbers(count):
    index = jnp.arange(count, dtype=jnp.int32)
    signed = jnp.where(index < count // 2, index, index - count)
    return signed.astype(jnp.float32) * (2.0 * math.pi / count)


def velocity_of(field, drift):
    spectrum = jnp.fft.fftn(field, axes=(1, 2, 3))
    wave_z = wave_numbers(NZ)[:, None, None]
    wave_y = wave_numbers(NY)[None, :, None]
    wave_x = wave_numbers(NX)[None, None, :]
    squared = wave_x * wave_x + wave_y * wave_y + wave_z * wave_z
    inverse = jnp.where(squared > 0, 1.0 / jnp.where(squared > 0, squared, 1.0), 0.0 * squared)
    stream = spectrum * inverse
    cross_x = wave_y * stream[2] - wave_z * stream[1]
    cross_y = wave_z * stream[0] - wave_x * stream[2]
    cross_z = wave_x * stream[1] - wave_y * stream[0]
    result = jnp.real(jnp.fft.ifftn(1j * jnp.stack([cross_x, cross_y, cross_z]), axes=(1, 2, 3)))
    return result + drift[:, None, None, None]


def central(values, axis):
    return (jnp.roll(values, -1, axis) - jnp.roll(values, 1, axis)) * 0.5


def stretch(field, speed, grad_x):
    grad_y = central(speed, 2)
    grad_z = central(speed, 1)
    return field + TIME_STEP * (field[0:1] * grad_x + field[1:2] * grad_y + field[2:3] * grad_z)


def remesh_periodic(values, shift, axis):
    total = jnp.zeros_like(values)
    for offset in range(-2, 3):
        total = total + jnp.roll(values, offset, axis) * kernel_weight(offset - jnp.roll(shift, offset, axis))
    return total


def remesh_inflow(values, shift, ghost_values, ghost_shift):
    q_ext = jnp.concatenate([ghost_values, values, jnp.zeros_like(values[..., :2])], -1)
    d_ext = jnp.concatenate([ghost_shift, shift, jnp.zeros_like(shift[..., :2])], -1)
    total = jnp.zeros_like(values)
    for offset in range(-2, 3):
        start = 2 - offset
        total = total + q_ext[..., start:start + NX] * kernel_weight(offset - d_ext[..., start:start + NX])
    return total


def reference(vorticity, wind):
    speed_pre = velocity_of(vorticity[0], wind[0])
    speed_wake = velocity_of(vorticity[1], wind[1])
    strength_pre = stretch(vorticity[0], speed_pre, central(speed_pre, 3))
    extended = jnp.concatenate([speed_pre[..., NX - 1:], speed_wake, speed_wake[..., NX - 1:]], -1)
    grad_wake = (extended[..., 2:] - extended[..., :-2]) * 0.5
    strength_wake = stretch(vorticity[1], speed_wake, grad_wake)
    moved_pre = remesh_periodic(strength_pre, TIME_STEP * speed_pre[0:1], 3)
    moved_wake = remesh_inflow(strength_wake, TIME_STEP * speed_wake[0:1], strength_pre[..., NX - 2:], TIME_STEP * speed_pre[0:1][..., NX - 2:])
    outputs = []
    for moved, speed in ((moved_pre, speed_pre), (moved_wake, speed_wake)):
        lateral = remesh_periodic(moved, TIME_STEP * speed[1:2], 2)
        outputs.append(remesh_periodic(lateral, TIME_STEP * speed[2:3], 1))
    return jnp.stack(outputs), jnp.stack([speed_pre, speed_wake])
```

```python
import functools
import math

import jax
import jax.numpy as jnp
import numpy as np
from jax import lax
from jax.experimental import pallas as pl
from jax.experimental.pallas import tpu as pltpu
from jax.sharding import PartitionSpec as P

TIME_STEP = 0.4
HIGH = lax.Precision.HIGH
BF16 = jnp.bfloat16
F32 = jnp.float32
VMEM_BYTES = 56 * 1024 * 1024
COLUMNS = 16


def shifted(value, axis, steps):
    count = lax.axis_size(axis)
    initial, last = (max(0, -steps), min(count, count - steps))
    return lax.ppermute(value, axis, [(source, source + steps) for source in range(initial, last)])


def rims(cells, axis, dim, width):
    count = lax.axis_size(axis)
    head = lax.slice_in_dim(cells, 0, width, axis=dim)
    tail = lax.slice_in_dim(cells, cells.shape[dim] - width, cells.shape[dim], axis=dim)
    low = lax.ppermute(tail, axis, [(i, (i + 1) % count) for i in range(count)])
    high = lax.ppermute(head, axis, [((i + 1) % count, i) for i in range(count)])
    return low, high


def rimmed(cells, sides, width):
    for axis, dim in sides:
        low, high = rims(cells, axis, dim, width)
        cells = jnp.concatenate([low, cells, high], axis=dim)
    return cells


def kernel_weight(offset):
    mag = jnp.abs(offset)
    inner = 1.0 - 2.5 * mag * mag + 1.5 * mag * mag * mag
    outer = 0.5 * (2.0 - mag) * (2.0 - mag) * (1.0 - mag)
    return jnp.where(mag < 1.0, inner, jnp.where(mag < 2.0, outer, 0.0 * mag))


def double_weight(offset):
    e = jnp.maximum(1.0 - jnp.abs(offset), -1.0)
    u = 1.0 + e
    p = jnp.maximum(e, 0.0)
    return u * u * e + p * p * (2.0 - 4.0 * p)


def angles(count):
    positions = np.arange(count)
    product = positions[:, None] * positions[None, :] % count
    angle = product * (2.0 * np.pi / count)
    return (np.cos(angle), np.sin(angle))


def complex_table(count, inverse):
    cosine, sine = angles(count)
    if inverse:
        cosine, sine = (cosine / count, -sine / count)
    rows_real = np.stack([cosine, -sine], 1)
    rows_imag = np.stack([sine, cosine], 1)
    return np.stack([rows_real, rows_imag], 0)


def halves(table):
    table = np.asarray(table, np.float32)
    high = np.asarray(table, BF16)
    low = np.asarray(table - high.astype(np.float32), BF16)
    return high, low


def split(value):
    high = value.astype(BF16)
    return high, (value - high.astype(F32)).astype(BF16)


def product(left, right, dims=(((1,), (0,)), ((), ()))):
    def one(a, b):
        return lax.dot_general(a, b, dims, preferred_element_type=F32)

    return one(left[0], right[0]) + (one(left[0], right[1]) + one(left[1], right[0]))


def wave(index, count, odd):
    signed = jnp.where(index < count // 2, index, index - count)
    if odd:
        signed = jnp.where(index == count // 2, 0, signed)
    return signed.astype(F32) * (2.0 * math.pi / count)


def middle_kernel(
    sizes, extra, base_ref, lines_ref, cos_h, cos_l, sin_h, sin_l, fwd_h, fwd_l, back_h, back_l, out_ref, spec, keep
):
    size_gy, size_gz, count_x = sizes
    local_z = lines_ref.shape[3]
    width = lines_ref.shape[4]
    count_z = local_z * size_gz
    count_y = spec.shape[2]
    step = pl.program_id(0)
    index_x = base_ref[0] + jnp.maximum(step - extra, 0)
    packed = index_x == 0
    top = jnp.logical_and(packed, step < extra)
    lane = lax.broadcasted_iota(jnp.int32, (count_z, size_gy * width), 1)
    is_real = (lane % width) < width // 2

    def plane():
        def forward(comp, carry):
            rows = []
            for y in range(size_gy):
                parts = [lines_ref[y * size_gz + z, 0, comp] for z in range(size_gz)]
                rows.append(jnp.concatenate(parts, 0))
            if extra:
                moved = [jnp.where(top, pltpu.roll(row, width // 2, 1), row) for row in rows]
                value = jnp.concatenate(moved, 1)
                value = jnp.where(jnp.logical_and(packed, jnp.logical_not(is_real)), 0.0, value)
            else:
                value = jnp.concatenate(rows, 1)
            value = product(split(value), (fwd_h[...], fwd_l[...]))
            real, imag = (split(value[:, :count_y]), split(value[:, count_y:]))
            cosine = (cos_h[...], cos_l[...])
            sine = (sin_h[...], sin_l[...])
            spec[comp] = product(cosine, real) + product(sine, imag)
            spec[3 + comp] = product(cosine, imag) - product(sine, real)
            return carry

        lax.fori_loop(0, 3, forward, 0)
        wave_x = wave(jnp.full((1, 1), index_x, jnp.int32), count_x, False)
        wave_x = jnp.where(top, math.pi, wave_x)
        curl_x = jnp.where(packed, 0.0, wave_x)
        tall = 64
        for first in range(0, count_z, tall):
            rows = pl.ds(first, tall)
            index_z = first + lax.broadcasted_iota(jnp.int32, (tall, 1), 0)
            index_y = lax.broadcasted_iota(jnp.int32, (1, count_y), 1)
            wave_z, wave_y = (wave(index_z, count_z, False), wave(index_y, count_y, False))
            curl_z, curl_y = (wave(index_z, count_z, True), wave(index_y, count_y, True))
            squared = wave_x * wave_x + wave_y * wave_y + wave_z * wave_z
            inverse = jnp.where(squared > 0, 1.0 / jnp.where(squared > 0, squared, 1.0), 0.0)
            inverse = inverse * (1.0 / count_z)
            for part, sign in ((3, -1.0), (0, 1.0)):
                scaled = inverse * sign
                s0, s1, s2 = [spec[part + comp, rows, :] * scaled for comp in range(3)]
                values = (curl_y * s2 - curl_z * s1, curl_z * s0 - curl_x * s2, curl_x * s1 - curl_y * s0)
                for comp in range(3):
                    spec[6 + (3 - part) + comp, rows, :] = values[comp]

        def backward(comp, carry):
            real, imag = (split(spec[6 + comp]), split(spec[9 + comp]))
            cosine = (cos_h[...], cos_l[...])
            sine = (sin_h[...], sin_l[...])
            value = jnp.concatenate(
                [
                    product(cosine, real) - product(sine, imag),
                    product(cosine, imag) + product(sine, real),
                ],
                1,
            )
            value = product(split(value), (back_h[...], back_l[...]))
            if extra:
                for y in range(size_gy):
                    cut = value[:, y * width : (y + 1) * width]

                    @pl.when(top)
                    def _():
                        keep[comp, :, y * width : (y + 1) * width] = pltpu.roll(cut, width // 2, 1)

                saved = keep[comp]
                merge = jnp.logical_and(packed, jnp.logical_not(is_real))
                value = jnp.where(merge, saved, value)
            for y in range(size_gy):
                for z in range(size_gz):
                    out_ref[y * size_gz + z, 0, comp] = value[
                        z * local_z : (z + 1) * local_z, y * width : (y + 1) * width
                    ]
            return carry

        lax.fori_loop(0, 3, backward, 0)

    if extra:
        pl.when(jnp.logical_or(step >= extra, packed))(plane)
    else:
        plane()


def middle(lines, base, tables, sizes, extra):
    size_gy, size_gz, count_x = sizes
    owners, share, _, local_z, width = lines.shape
    count_z = local_z * size_gz
    count_y = size_gy * width // 2
    shape = (owners, 1, 3, local_z, width)

    def at(step, base_ref):
        return (0, jnp.maximum(step - extra, 0), 0, 0, 0)

    def whole(table):
        return pl.BlockSpec(table.shape, lambda step, base_ref: (0, 0))

    flops = (share + extra) * 3 * 4 * 2 * 3 * count_z * (2 * count_y) ** 2
    return pl.pallas_call(
        functools.partial(middle_kernel, sizes, extra),
        grid_spec=pltpu.PrefetchScalarGridSpec(
            num_scalar_prefetch=1,
            grid=(share + extra,),
            in_specs=[pl.BlockSpec(shape, at)] + [whole(t) for t in tables],
            out_specs=pl.BlockSpec(shape, at),
            scratch_shapes=[
                pltpu.VMEM((12, count_z, count_y), F32),
                pltpu.VMEM((3, count_z, 2 * count_y) if extra else (1, 8, 128), F32),
            ],
        ),
        out_shape=jax.ShapeDtypeStruct(lines.shape, F32),
        compiler_params=pltpu.CompilerParams(
            dimension_semantics=("arbitrary",), vmem_limit_bytes=VMEM_BYTES
        ),
        cost_estimate=pl.CostEstimate(flops=flops, bytes_accessed=lines.size * 8, transcendentals=0),
        name="middle",
    )(base, lines, *tables)


def speed_kernel(chunks, tall, drift_ref, *refs):
    lines = refs[:chunks]
    table_h, table_l, thin_h, thin_l, out_ref, thin_ref = refs[chunks:]
    width = lines[0].shape[3]
    half = width // 2
    comp = pl.program_id(0)
    rows = []
    for z in range(tall):
        value = jnp.concatenate([ref[:, 0, z, :] for ref in lines], 0)
        turned = value.T
        rows.append(jnp.concatenate([turned[:half], turned[half:]], 1))
    left = split(jnp.concatenate(rows, 0))
    value = product(left, (table_h[...], table_l[...])) + drift_ref[comp]
    out_ref[0] = value.reshape(tall, half, value.shape[1])
    contract = (((1,), (1,)), ((), ()))
    thin_ref[0] = product((thin_h[...], thin_l[...]), left, contract) + drift_ref[comp]


def speed(parts, drift, tables):
    chunks = len(parts)
    depth, _, local_z, width = parts[0].shape
    count_x = tables[0].shape[1]
    half = width // 2
    tall = 8
    return pl.pallas_call(
        functools.partial(speed_kernel, chunks, tall),
        grid_spec=pltpu.PrefetchScalarGridSpec(
            num_scalar_prefetch=1,
            grid=(3, local_z // tall),
            in_specs=[pl.BlockSpec((depth, 1, tall, width), lambda c, z, d: (0, c, z, 0))] * chunks
            + [pl.BlockSpec(t.shape, lambda c, z, d: (0, 0)) for t in tables],
            out_specs=[
                pl.BlockSpec((1, tall, half, count_x), lambda c, z, d: (c, z, 0, 0)),
                pl.BlockSpec((1, 8, tall * half), lambda c, z, d: (c, 0, z)),
            ],
        ),
        out_shape=[
            jax.ShapeDtypeStruct((3, local_z, half, count_x), F32),
            jax.ShapeDtypeStruct((3, 8, local_z * half), F32),
        ],
        compiler_params=pltpu.CompilerParams(
            dimension_semantics=("arbitrary", "arbitrary"), vmem_limit_bytes=VMEM_BYTES
        ),
        cost_estimate=pl.CostEstimate(
            flops=6 * 3 * local_z * half * count_x * 2 * count_x // 2,
            bytes_accessed=24 * local_z * half * count_x,
            transcendentals=0,
        ),
        name="speed",
    )(drift, *parts, *tables)


def remesh_kernel(
    wake_ref, v_ref, vl_ref, vh_ref, vzl_ref, vzh_ref, f_ref, fl_ref, fh_ref, fzl_ref, fzh_ref,
    ghost_ref, pick_ref, out_ref, speeds, field, moved, ghosts, total,
):
    local_y, count_x = v_ref.shape[2:]
    step = pl.program_id(0)
    local_z = pl.num_programs(0) - 6
    wake = wake_ref[0] == 1
    edge = 8
    here = step % 3

    @pl.when(step == 0)
    def _():
        speeds[...] = jnp.zeros_like(speeds)
        field[...] = jnp.zeros_like(field)
        total[...] = jnp.zeros_like(total)

    @pl.when(step < 3)
    def _():
        speeds[here, :, edge - 4 : edge + local_y + 4] = vzl_ref[:, 0]

    @pl.when(step >= local_z + 3)
    def _():
        speeds[here, :, edge - 4 : edge + local_y + 4] = vzh_ref[:, 0]

    @pl.when(jnp.logical_and(step >= 3, step < local_z + 3))
    def _():
        speeds[here, :, edge - 4 : edge] = vl_ref[:, 0]
        speeds[here, :, edge : edge + local_y] = v_ref[:, 0]
        speeds[here, :, edge + local_y : edge + local_y + 4] = vh_ref[:, 0]

    @pl.when(step < 4)
    def _():
        field[:, edge - 2 : edge + local_y + 2] = fzl_ref[:, 0]

    @pl.when(step >= local_z + 4)
    def _():
        field[:, edge - 2 : edge + local_y + 2] = fzh_ref[:, 0]

    @pl.when(jnp.logical_and(step >= 4, step < local_z + 4))
    def _():
        field[:, edge - 2 : edge] = fl_ref[:, 0]
        field[:, edge : edge + local_y] = f_ref[:, 0]
        field[:, edge + local_y : edge + local_y + 2] = fh_ref[:, 0]

    @pl.when(step >= 2)
    def _():
        now, before = ((step + 2) % 3, (step + 1) % 3)
        ghosts[...] = lax.dot_general(
            ghost_ref[0], pick_ref[...], (((0,), (0,)), ((), ())),
            preferred_element_type=F32, precision=lax.Precision.HIGHEST,
        )
        lane = lax.broadcasted_iota(jnp.int32, (8, count_x), 1)
        first = jnp.logical_and(lane == 0, wake)
        last = jnp.logical_and(lane == count_x - 1, wake)
        cut = {
            offset: jnp.logical_and(lane >= count_x - offset if offset > 0 else lane < -offset, wake)
            for offset in (-2, -1, 1, 2)
        }
        total_rows = local_y + 2 * edge

        def wide(value):
            return jnp.concatenate([value, jnp.zeros((8, count_x - 128), F32)], 1)

        for row in range(0, total_rows, 8):
            rows = slice(row, row + 8)
            vel = [speeds[now, comp, rows] for comp in range(3)]
            vor = [field[comp, rows] * 0.125 for comp in range(3)]
            strength = []
            for comp in range(3):
                v = vel[comp]
                left = pltpu.roll(v, 1, 1)
                ghost = wide(ghosts[rows, comp * 128 : (comp + 1) * 128])
                left = jnp.where(first, ghost, left)
                right = jnp.where(last, v, pltpu.roll(v, count_x - 1, 1))
                if row == 0:
                    down = pltpu.roll(v, 1, 0)
                else:
                    down = speeds[now, comp, row - 1 : row + 7]
                if row == total_rows - 8:
                    up = pltpu.roll(v, 7, 0)
                else:
                    up = speeds[now, comp, row + 1 : row + 9]
                away = speeds[here, comp, rows] - speeds[before, comp, rows]
                pulled = vor[0] * (right - left) + vor[1] * (up - down) + vor[2] * away
                strength.append(vor[comp] + (0.5 * TIME_STEP) * pulled)
            shift = TIME_STEP * vel[0]
            sums = [strength[comp] * double_weight(-shift) for comp in range(3)]
            for offset in (-2, -1, 1, 2):
                weight = jnp.where(cut[offset], 0.0, double_weight(offset - shift))
                for comp in range(3):
                    sums[comp] += pltpu.roll(strength[comp] * weight, offset % count_x, 1)
            for comp in range(3):
                extra = ghosts[rows, (3 + comp) * 128 : (4 + comp) * 128]
                moved[comp, rows] = sums[comp] + wide(extra)
        for row in range(edge, edge + local_y, 8):
            lateral = [0.0, 0.0, 0.0]
            for offset in range(-2, 3):
                rows = slice(row - offset, row - offset + 8)
                weight = double_weight(offset - TIME_STEP * speeds[now, 1, rows])
                for comp in range(3):
                    lateral[comp] += moved[comp, rows] * weight
            shift = TIME_STEP * speeds[now, 2, row : row + 8]
            rows = slice(row - edge, row - edge + 8)
            for offset in range(-2, 3):
                weight = double_weight(offset - shift)
                slot = (step + 5 + offset) % 5
                for comp in range(3):
                    term = lateral[comp] * weight
                    if offset == -2:
                        out_ref[comp, 0, rows] = total[slot, comp, rows] + term
                    elif offset == 2:
                        total[slot, comp, rows] = term
                    else:
                        total[slot, comp, rows] += term


def remesh(wake, v, v_rims, f, f_rims, ghost, pick):
    _, local_z, local_y, count_x = v.shape
    steps = local_z + 6
    tall = local_y + 16

    def plane(rows, delay, limit):
        return pl.BlockSpec(
            (3, 1, rows, count_x), lambda i, w: (0, jnp.clip(i - delay, 0, limit - 1), 0, 0)
        )

    in_specs = [
        plane(local_y, 3, local_z),
        plane(4, 3, local_z),
        plane(4, 3, local_z),
        plane(local_y + 8, 0, 3),
        plane(local_y + 8, local_z + 3, 3),
        plane(local_y, 4, local_z),
        plane(2, 4, local_z),
        plane(2, 4, local_z),
        plane(local_y + 4, 2, 2),
        plane(local_y + 4, local_z + 4, 2),
        pl.BlockSpec((1, COLUMNS, tall), lambda i, w: (jnp.clip(i - 2, 0, local_z + 3), 0, 0)),
        pl.BlockSpec(pick.shape, lambda i, w: (0, 0)),
    ]
    return pl.pallas_call(
        remesh_kernel,
        grid_spec=pltpu.PrefetchScalarGridSpec(
            num_scalar_prefetch=1,
            grid=(steps,),
            in_specs=in_specs,
            out_specs=pl.BlockSpec(
                (3, 1, local_y, count_x), lambda i, w: (0, jnp.clip(i - 6, 0, local_z - 1), 0, 0)
            ),
            scratch_shapes=[
                pltpu.VMEM((3, 3, tall, count_x), F32),
                pltpu.VMEM((3, tall, count_x), F32),
                pltpu.VMEM((3, tall, count_x), F32),
                pltpu.VMEM((tall, 6 * 128), F32),
                pltpu.VMEM((5, 3, local_y, count_x), F32),
            ],
        ),
        out_shape=jax.ShapeDtypeStruct(v.shape, F32),
        compiler_params=pltpu.CompilerParams(
            dimension_semantics=("arbitrary",), vmem_limit_bytes=VMEM_BYTES
        ),
        cost_estimate=pl.CostEstimate(flops=v.size * 150, bytes_accessed=v.size * 12, transcendentals=0),
        name="remesh",
    )(wake, v, *v_rims, f, *f_rims, ghost, pick)


def all_rims(cells, rows, planes):
    low, high = rims(cells, "gy", 2, rows)
    local_z = cells.shape[1]
    ends = []
    for part in (slice(local_z - planes, local_z), slice(0, planes)):
        ends.append(jnp.concatenate([low[:, part], cells[:, part], high[:, part]], 2))
    count = lax.axis_size("gz")
    z_low = lax.ppermute(ends[0], "gz", [(i, (i + 1) % count) for i in range(count)])
    z_high = lax.ppermute(ends[1], "gz", [((i + 1) % count, i) for i in range(count)])
    return low, high, z_low, z_high


def ghost_columns(field_planes, thin):
    inner = thin[:, :, 1:-1, 1:-1]
    grad_z = (thin[:, 1:3, 2:, 1:-1] - thin[:, 1:3, :-2, 1:-1]) * 0.5
    grad_y = (thin[:, 1:3, 1:-1, 2:] - thin[:, 1:3, 1:-1, :-2]) * 0.5
    grad_x = (inner[:, 2:4] - inner[:, 0:2]) * 0.5
    pulled = field_planes[0:1] * grad_x + field_planes[1:2] * grad_y + field_planes[2:3] * grad_z
    strength = field_planes + TIME_STEP * pulled
    shift = TIME_STEP * inner[0, 1:3]
    zero = strength[:, 0] * kernel_weight(2.0 - shift[0]) + strength[:, 1] * kernel_weight(1.0 - shift[1])
    one = strength[:, 1] * kernel_weight(2.0 - shift[1])
    columns = jnp.concatenate([inner[:, 2], zero, one], 0)
    columns = jnp.pad(columns, ((0, COLUMNS - columns.shape[0]), (0, 0), (6, 6)))
    return columns.transpose(1, 0, 2)


def body(vorticity, wind):
    field = vorticity[0]
    drift = wind[0]
    count_x = field.shape[3]
    half_x = count_x // 2
    size_gy = lax.axis_size("gy")
    size_gz = lax.axis_size("gz")
    owners = size_gy * size_gz
    local_z, local_y = field.shape[1:3]
    count_y = local_y * size_gy
    count_z = local_z * size_gz
    share = half_x // owners
    chunks = math.gcd(share, 4)
    part = share // chunks
    sizes = (size_gy, size_gz, count_x)
    wake = lax.axis_index("grp").astype(jnp.int32).reshape(1)
    owner = lax.axis_index("gy") * size_gz + lax.axis_index("gz")

    cosine_x, sine_x = angles(count_x)
    alternate = 1.0 - 2.0 * (np.arange(count_x) % 2)
    forward_cos = cosine_x[:, :half_x]
    forward_sin = np.concatenate([alternate[:, None], -sine_x[:, 1:half_x]], 1)
    back_cos = np.concatenate([cosine_x[:1], 2.0 * cosine_x[1:half_x]], 0) / count_x
    back_sin = np.concatenate([-alternate[None, :], 2.0 * sine_x[1:half_x]], 0) / -count_x

    table_y = complex_table(count_y, False)
    table_y = table_y.reshape(2, size_gy, local_y, 2 * count_y)
    table_y = table_y.transpose(1, 0, 2, 3).reshape(2 * count_y, 2 * count_y)
    back_y = complex_table(count_y, True)
    back_y = back_y.reshape(2 * count_y, 2, size_gy, local_y)
    back_y = back_y.transpose(0, 2, 1, 3).reshape(2 * count_y, 2 * count_y)
    cosine_z, sine_z = angles(count_z)
    tables = [jnp.asarray(h) for t in (cosine_z, sine_z, table_y, back_y) for h in halves(t)]

    def dot(letters, values, table):
        return jnp.einsum(letters, values, jnp.asarray(table, F32), precision=HIGH)

    pieces = []
    for chunk in range(chunks):
        def pick(table):
            return table.reshape(count_x, owners, chunks, part)[:, :, chunk].reshape(count_x, -1)

        lines = jnp.concatenate(
            [
                dot("czyx,xk->kczy", field, pick(forward_cos)),
                dot("czyx,xk->kczy", field, pick(forward_sin)),
            ],
            3,
        )
        pieces.append(lax.all_to_all(lines, ("gy", "gz"), split_axis=0, concat_axis=0, tiled=True))

    field_rims = all_rims(field, 2, 2)
    field_planes = rimmed(
        field[..., count_x - 2 :].transpose(0, 3, 1, 2), (("gy", 3), ("gz", 2)), 2
    )

    parts = []
    for chunk in range(chunks):
        base = (owner * share + chunk * part).astype(jnp.int32).reshape(1)
        lines = pieces[chunk].reshape(owners, part, 3, local_z, 2 * local_y)
        lines = middle(lines, base, tables, sizes, 1 if chunk == 0 else 0)
        lines = lines.reshape(owners * part, 3, local_z, 2 * local_y)
        parts.append(lax.all_to_all(lines, ("gy", "gz"), split_axis=0, concat_axis=0, tiled=True))

    def turned(table):
        return table.reshape(owners, chunks, part, -1).transpose(1, 0, 2, 3).reshape(half_x, -1)

    back = np.concatenate([turned(back_cos), turned(back_sin)], 0)
    thin = np.zeros((8, count_x))
    thin[:4] = back[:, [count_x - 3, count_x - 2, count_x - 1, 0]].T
    speed_tables = [jnp.asarray(h) for t in (back, thin) for h in halves(t)]
    velocity, thin = speed(parts, drift, speed_tables)

    velocity_rims = all_rims(velocity, 4, 3)
    thin = thin.reshape(3, 8, local_z, local_y)[:, :4]
    thin = rimmed(thin, (("gy", 3), ("gz", 2)), 3)
    ghost = shifted(ghost_columns(field_planes, thin), "grp", 1)
    choose = np.zeros((COLUMNS, 6, 128), np.float32)
    for comp in range(3):
        choose[comp, comp, 0] = 1.0
        choose[3 + comp, 3 + comp, 0] = 0.25
        choose[6 + comp, 3 + comp, 1] = 0.25
    choose = jnp.asarray(choose.reshape(COLUMNS, 6 * 128))
    result = remesh(wake, velocity, velocity_rims, field, field_rims, ghost, choose)
    return (result[None], velocity[None])


def solution(mesh):
    return jax.shard_map(
        body,
        mesh=mesh,
        in_specs=(P("grp", None, "gz", "gy", None), P("grp", None)),
        out_specs=(P("grp", None, "gz", "gy", None), P("grp", None, "gz", "gy", None)),
        check_vma=False,
    )
```

```python
import functools
import math

import jax
import jax.numpy as jnp
import numpy as np
from jax import lax
from jax.experimental import pallas as pl
from jax.experimental.pallas import tpu as pltpu
from jax.sharding import PartitionSpec as P

TIME_STEP = 0.4
HIGH = lax.Precision.HIGH
BF16 = jnp.bfloat16
F32 = jnp.float32
VMEM_BYTES = 56 * 1024 * 1024
COLUMNS = 16


def shifted(value, axis, steps):
    count = lax.axis_size(axis)
    initial, last = (max(0, -steps), min(count, count - steps))
    return lax.ppermute(value, axis, [(source, source + steps) for source in range(initial, last)])


def rims(cells, axis, dim, width):
    count = lax.axis_size(axis)
    head = lax.slice_in_dim(cells, 0, width, axis=dim)
    tail = lax.slice_in_dim(cells, cells.shape[dim] - width, cells.shape[dim], axis=dim)
    low = lax.ppermute(tail, axis, [(i, (i + 1) % count) for i in range(count)])
    high = lax.ppermute(head, axis, [((i + 1) % count, i) for i in range(count)])
    return low, high


def rimmed(cells, sides, width):
    for axis, dim in sides:
        low, high = rims(cells, axis, dim, width)
        cells = jnp.concatenate([low, cells, high], axis=dim)
    return cells


def kernel_weight(offset):
    mag = jnp.abs(offset)
    inner = 1.0 - 2.5 * mag * mag + 1.5 * mag * mag * mag
    outer = 0.5 * (2.0 - mag) * (2.0 - mag) * (1.0 - mag)
    return jnp.where(mag < 1.0, inner, jnp.where(mag < 2.0, outer, 0.0 * mag))


def double_weight(offset):
    e = jnp.maximum(1.0 - jnp.abs(offset), -1.0)
    u = 1.0 + e
    p = jnp.maximum(e, 0.0)
    return u * u * e + p * p * (2.0 - 4.0 * p)


def angles(count):
    positions = np.arange(count)
    product = positions[:, None] * positions[None, :] % count
    angle = product * (2.0 * np.pi / count)
    return (np.cos(angle), np.sin(angle))


def complex_table(count, inverse):
    cosine, sine = angles(count)
    if inverse:
        cosine, sine = (cosine / count, -sine / count)
    rows_real = np.stack([cosine, -sine], 1)
    rows_imag = np.stack([sine, cosine], 1)
    return np.stack([rows_real, rows_imag], 0)


def halves(table):
    table = np.asarray(table, np.float32)
    high = np.asarray(table, BF16)
    low = np.asarray(table - high.astype(np.float32), BF16)
    return high, low


def split(value):
    high = value.astype(BF16)
    return high, (value - high.astype(F32)).astype(BF16)


def product(left, right, dims=(((1,), (0,)), ((), ()))):
    def one(a, b):
        return lax.dot_general(a, b, dims, preferred_element_type=F32)

    return one(left[0], right[0]) + (one(left[0], right[1]) + one(left[1], right[0]))


def wave(index, count, odd):
    signed = jnp.where(index < count // 2, index, index - count)
    if odd:
        signed = jnp.where(index == count // 2, 0, signed)
    return signed.astype(F32) * (2.0 * math.pi / count)


def middle_kernel(
    sizes, extra, base_ref, lines_ref, cos_h, cos_l, sin_h, sin_l, fwd_h, fwd_l, back_h, back_l, out_ref, spec, keep
):
    size_gy, size_gz, count_x = sizes
    local_z = lines_ref.shape[3]
    width = lines_ref.shape[4]
    count_z = local_z * size_gz
    count_y = spec.shape[2]
    step = pl.program_id(0)
    index_x = base_ref[0] + jnp.maximum(step - extra, 0)
    packed = index_x == 0
    top = jnp.logical_and(packed, step < extra)
    lane = lax.broadcasted_iota(jnp.int32, (count_z, size_gy * width), 1)
    is_real = (lane % width) < width // 2

    def plane():
        def forward(comp, carry):
            rows = []
            for y in range(size_gy):
                parts = [lines_ref[y * size_gz + z, 0, comp] for z in range(size_gz)]
                rows.append(jnp.concatenate(parts, 0))
            if extra:
                moved = [jnp.where(top, pltpu.roll(row, width // 2, 1), row) for row in rows]
                value = jnp.concatenate(moved, 1)
                value = jnp.where(jnp.logical_and(packed, jnp.logical_not(is_real)), 0.0, value)
            else:
                value = jnp.concatenate(rows, 1)
            value = product(split(value), (fwd_h[...], fwd_l[...]))
            real, imag = (split(value[:, :count_y]), split(value[:, count_y:]))
            cosine = (cos_h[...], cos_l[...])
            sine = (sin_h[...], sin_l[...])
            spec[comp] = product(cosine, real) + product(sine, imag)
            spec[3 + comp] = product(cosine, imag) - product(sine, real)
            return carry

        lax.fori_loop(0, 3, forward, 0)
        wave_x = wave(jnp.full((1, 1), index_x, jnp.int32), count_x, False)
        wave_x = jnp.where(top, math.pi, wave_x)
        curl_x = jnp.where(packed, 0.0, wave_x)
        tall = 64
        for first in range(0, count_z, tall):
            rows = pl.ds(first, tall)
            index_z = first + lax.broadcasted_iota(jnp.int32, (tall, 1), 0)
            index_y = lax.broadcasted_iota(jnp.int32, (1, count_y), 1)
            wave_z, wave_y = (wave(index_z, count_z, False), wave(index_y, count_y, False))
            curl_z, curl_y = (wave(index_z, count_z, True), wave(index_y, count_y, True))
            squared = wave_x * wave_x + wave_y * wave_y + wave_z * wave_z
            inverse = jnp.where(squared > 0, 1.0 / jnp.where(squared > 0, squared, 1.0), 0.0)
            inverse = inverse * (1.0 / count_z)
            for part, sign in ((3, -1.0), (0, 1.0)):
                scaled = inverse * sign
                s0, s1, s2 = [spec[part + comp, rows, :] * scaled for comp in range(3)]
                values = (curl_y * s2 - curl_z * s1, curl_z * s0 - curl_x * s2, curl_x * s1 - curl_y * s0)
                for comp in range(3):
                    spec[6 + (3 - part) + comp, rows, :] = values[comp]

        def backward(comp, carry):
            real, imag = (split(spec[6 + comp]), split(spec[9 + comp]))
            cosine = (cos_h[...], cos_l[...])
            sine = (sin_h[...], sin_l[...])
            value = jnp.concatenate(
                [
                    product(cosine, real) - product(sine, imag),
                    product(cosine, imag) + product(sine, real),
                ],
                1,
            )
            value = product(split(value), (back_h[...], back_l[...]))
            if extra:
                for y in range(size_gy):
                    cut = value[:, y * width : (y + 1) * width]

                    @pl.when(top)
                    def _():
                        keep[comp, :, y * width : (y + 1) * width] = pltpu.roll(cut, width // 2, 1)

                saved = keep[comp]
                merge = jnp.logical_and(packed, jnp.logical_not(is_real))
                value = jnp.where(merge, saved, value)
            for y in range(size_gy):
                for z in range(size_gz):
                    out_ref[y * size_gz + z, 0, comp] = value[
                        z * local_z : (z + 1) * local_z, y * width : (y + 1) * width
                    ]
            return carry

        lax.fori_loop(0, 3, backward, 0)

    if extra:
        pl.when(jnp.logical_or(step >= extra, packed))(plane)
    else:
        plane()


def middle(lines, base, tables, sizes, extra):
    size_gy, size_gz, count_x = sizes
    owners, share, _, local_z, width = lines.shape
    count_z = local_z * size_gz
    count_y = size_gy * width // 2
    shape = (owners, 1, 3, local_z, width)

    def at(step, base_ref):
        return (0, jnp.maximum(step - extra, 0), 0, 0, 0)

    def whole(table):
        return pl.BlockSpec(table.shape, lambda step, base_ref: (0, 0))

    flops = (share + extra) * 3 * 4 * 2 * 3 * count_z * (2 * count_y) ** 2
    return pl.pallas_call(
        functools.partial(middle_kernel, sizes, extra),
        grid_spec=pltpu.PrefetchScalarGridSpec(
            num_scalar_prefetch=1,
            grid=(share + extra,),
            in_specs=[pl.BlockSpec(shape, at)] + [whole(t) for t in tables],
            out_specs=pl.BlockSpec(shape, at),
            scratch_shapes=[
                pltpu.VMEM((12, count_z, count_y), F32),
                pltpu.VMEM((3, count_z, 2 * count_y) if extra else (1, 8, 128), F32),
            ],
        ),
        out_shape=jax.ShapeDtypeStruct(lines.shape, F32),
        compiler_params=pltpu.CompilerParams(
            dimension_semantics=("arbitrary",), vmem_limit_bytes=VMEM_BYTES
        ),
        cost_estimate=pl.CostEstimate(flops=flops, bytes_accessed=lines.size * 8, transcendentals=0),
        name="middle",
    )(base, lines, *tables)


def planes_kernel(choose_ref, field_ref, out_ref):
    _, tall, local_y, width = field_ref.shape
    rows = field_ref[0].reshape(tall * local_y, width)
    out_ref[0] = lax.dot_general(
        choose_ref[...], rows, (((1,), (1,)), ((), ())),
        preferred_element_type=F32, precision=lax.Precision.HIGHEST,
    )


def last_planes(field):
    _, local_z, local_y, count_x = field.shape
    tall = 8
    choose = np.zeros((8, 128), np.float32)
    choose[0, 126] = 1.0
    choose[1, 127] = 1.0
    planes = pl.pallas_call(
        planes_kernel,
        grid=(3, local_z // tall),
        in_specs=[
            pl.BlockSpec((8, 128), lambda c, z: (0, 0)),
            pl.BlockSpec((1, tall, local_y, 128), lambda c, z: (c, z, 0, count_x // 128 - 1)),
        ],
        out_specs=pl.BlockSpec((1, 8, tall * local_y), lambda c, z: (c, 0, z)),
        out_shape=jax.ShapeDtypeStruct((3, 8, local_z * local_y), F32),
        compiler_params=pltpu.CompilerParams(dimension_semantics=("arbitrary", "arbitrary")),
        cost_estimate=pl.CostEstimate(flops=field.size * 400, bytes_accessed=field.size * 2, transcendentals=0),
        name="planes",
    )(jnp.asarray(choose), field)
    return planes[:, :2].reshape(3, 2, local_z, local_y)


def block_rows(lines, tall):
    rows = []
    for z in range(tall):
        rows.append(jnp.concatenate([ref[:, 0, z, :] for ref in lines], 0))
    return rows


def speed_kernel(chunks, tall, drift_ref, *refs):
    lines = refs[:chunks]
    table_h, table_l, out_ref = refs[chunks:]
    half = lines[0].shape[3] // 2
    rows = []
    for value in block_rows(lines, tall):
        turned = value.T
        rows.append(jnp.concatenate([turned[:half], turned[half:]], 1))
    left = split(jnp.concatenate(rows, 0))
    value = product(left, (table_h[...], table_l[...])) + drift_ref[pl.program_id(0)]
    out_ref[0] = value.reshape(tall, half, value.shape[1])


def edge_kernel(chunks, tall, drift_ref, *refs):
    lines = refs[:chunks]
    table_h, table_l, thin_h, thin_l, rows_ref, ends_ref, thin_ref = refs[chunks:]
    half = lines[0].shape[3] // 2
    drift = drift_ref[pl.program_id(0)]
    step = pl.program_id(1)
    blocks = block_rows(lines, tall)
    turned = [value.T for value in blocks]
    thin = (thin_h[...], thin_l[...])
    flat = []
    for value in blocks:
        both = product(thin, split(value))
        flat.append(both[:8, :half] + both[8:, half:])
    thin_ref[0] = jnp.concatenate(flat, 1) + drift
    table = (table_h[...], table_l[...])
    rows = []
    for value in turned:
        real = jnp.concatenate([value[:4], value[half - 4 : half]], 0)
        imag = jnp.concatenate([value[half : half + 4], value[2 * half - 4 :]], 0)
        rows.append(jnp.concatenate([real, imag], 1))
    value = product(split(jnp.concatenate(rows, 0)), table) + drift
    rows_ref[0] = value.reshape(tall, 8, value.shape[1])

    @pl.when(jnp.logical_or(step == 0, step == pl.num_programs(1) - 1))
    def _():
        whole = [jnp.concatenate([value[:half], value[half:]], 1) for value in turned]
        ends = product(split(jnp.concatenate(whole, 0)), table) + drift
        ends_ref[0] = ends.reshape(tall, half, ends.shape[1])


def speed(parts, drift, table, thin):
    chunks = len(parts)
    depth, _, local_z, width = parts[0].shape
    count_x = table[0].shape[1]
    half = width // 2
    tall = 8
    steps = local_z // tall
    params = pltpu.CompilerParams(
        dimension_semantics=("arbitrary", "arbitrary"), vmem_limit_bytes=VMEM_BYTES
    )
    line_specs = [pl.BlockSpec((depth, 1, tall, width), lambda c, z, d: (0, c, z, 0))] * chunks

    def whole(tables):
        return [pl.BlockSpec(t.shape, lambda c, z, d: (0, 0)) for t in tables]

    ends = min(2, steps)
    edges = pl.pallas_call(
        functools.partial(edge_kernel, chunks, tall),
        grid_spec=pltpu.PrefetchScalarGridSpec(
            num_scalar_prefetch=1,
            grid=(3, steps),
            in_specs=line_specs + whole(table) + whole(thin),
            out_specs=[
                pl.BlockSpec((1, tall, 8, count_x), lambda c, z, d: (c, z, 0, 0)),
                pl.BlockSpec((1, tall, half, count_x), lambda c, z, d: (c, (z + 1) // steps * (ends - 1), 0, 0)),
                pl.BlockSpec((1, 8, tall * half), lambda c, z, d: (c, 0, z)),
            ],
        ),
        out_shape=[
            jax.ShapeDtypeStruct((3, local_z, 8, count_x), F32),
            jax.ShapeDtypeStruct((3, ends * tall, half, count_x), F32),
            jax.ShapeDtypeStruct((3, 8, local_z * half), F32),
        ],
        compiler_params=params,
        cost_estimate=pl.CostEstimate(
            flops=3 * local_z * half * count_x * 800, bytes_accessed=16 * local_z * half * count_x, transcendentals=0
        ),
        name="edges",
    )(drift, *parts, *table, *thin)
    velocity = pl.pallas_call(
        functools.partial(speed_kernel, chunks, tall),
        grid_spec=pltpu.PrefetchScalarGridSpec(
            num_scalar_prefetch=1,
            grid=(3, steps),
            in_specs=line_specs + whole(table),
            out_specs=pl.BlockSpec((1, tall, half, count_x), lambda c, z, d: (c, z, 0, 0)),
        ),
        out_shape=jax.ShapeDtypeStruct((3, local_z, half, count_x), F32),
        compiler_params=params,
        cost_estimate=pl.CostEstimate(
            flops=3 * local_z * half * count_x * 8000, bytes_accessed=24 * local_z * half * count_x, transcendentals=0
        ),
        name="speed",
    )(drift, *parts, *table)
    return velocity, edges


def remesh_kernel(
    wake_ref, v_ref, vl_ref, vh_ref, vzl_ref, vzh_ref, f_ref, fl_ref, fh_ref, fzl_ref, fzh_ref,
    ghost_ref, pick_ref, out_ref, speeds, field, moved, ghosts, total,
):
    local_y, count_x = v_ref.shape[2:]
    step = pl.program_id(0)
    local_z = pl.num_programs(0) - 6
    wake = wake_ref[0] == 1
    edge = 8
    here = step % 3

    @pl.when(step == 0)
    def _():
        speeds[...] = jnp.zeros_like(speeds)
        field[...] = jnp.zeros_like(field)
        total[...] = jnp.zeros_like(total)

    @pl.when(step < 3)
    def _():
        speeds[here, :, edge - 4 : edge + local_y + 4] = vzl_ref[:, 0]

    @pl.when(step >= local_z + 3)
    def _():
        speeds[here, :, edge - 4 : edge + local_y + 4] = vzh_ref[:, 0]

    @pl.when(jnp.logical_and(step >= 3, step < local_z + 3))
    def _():
        speeds[here, :, edge - 4 : edge] = vl_ref[:, 0]
        speeds[here, :, edge : edge + local_y] = v_ref[:, 0]
        speeds[here, :, edge + local_y : edge + local_y + 4] = vh_ref[:, 0]

    @pl.when(step < 4)
    def _():
        field[:, edge - 2 : edge + local_y + 2] = fzl_ref[:, 0]

    @pl.when(step >= local_z + 4)
    def _():
        field[:, edge - 2 : edge + local_y + 2] = fzh_ref[:, 0]

    @pl.when(jnp.logical_and(step >= 4, step < local_z + 4))
    def _():
        field[:, edge - 2 : edge] = fl_ref[:, 0]
        field[:, edge : edge + local_y] = f_ref[:, 0]
        field[:, edge + local_y : edge + local_y + 2] = fh_ref[:, 0]

    @pl.when(step >= 2)
    def _():
        now, before = ((step + 2) % 3, (step + 1) % 3)
        picked = lax.dot_general(
            ghost_ref[0], pick_ref[...], (((0,), (0,)), ((), ())),
            preferred_element_type=F32, precision=lax.Precision.HIGHEST,
        )
        for part in range(6):
            ghosts[part] = picked[:, part * 128 : (part + 1) * 128]
        lane = lax.broadcasted_iota(jnp.int32, (8, count_x), 1)
        first = jnp.logical_and(lane == 0, wake)
        last = jnp.logical_and(lane == count_x - 1, wake)
        cut = {
            offset: jnp.logical_and(lane >= count_x - offset if offset > 0 else lane < -offset, wake)
            for offset in (-2, -1, 1, 2)
        }
        total_rows = local_y + 2 * edge

        def wide(value):
            return jnp.concatenate([value, jnp.zeros((8, count_x - 128), F32)], 1)

        def read(ref, index, row, away):
            if row:
                return ref[(*index, slice(row + away, row + away + 8))]
            parts = (slice(4 + away, 8 + away), slice(total_rows - 8 + away, total_rows - 4 + away))
            return jnp.concatenate([ref[(*index, part)] for part in parts], 0)

        for row in range(0, total_rows - 8, 8):
            vel = [read(speeds, (now, comp), row, 0) for comp in range(3)]
            vor = [read(field, (comp,), row, 0) * 0.125 for comp in range(3)]
            strength = []
            for comp in range(3):
                v = vel[comp]
                left = pltpu.roll(v, 1, 1)
                ghost = wide(read(ghosts, (comp,), row, 0))
                left = jnp.where(first, ghost, left)
                right = jnp.where(last, v, pltpu.roll(v, count_x - 1, 1))
                down = read(speeds, (now, comp), row, -1)
                up = read(speeds, (now, comp), row, 1)
                away = read(speeds, (here, comp), row, 0) - read(speeds, (before, comp), row, 0)
                pulled = vor[0] * (right - left) + vor[1] * (up - down) + vor[2] * away
                strength.append(vor[comp] + (0.5 * TIME_STEP) * pulled)
            shift = TIME_STEP * vel[0]
            sums = [strength[comp] * double_weight(-shift) for comp in range(3)]
            for offset in (-2, -1, 1, 2):
                weight = jnp.where(cut[offset], 0.0, double_weight(offset - shift))
                for comp in range(3):
                    sums[comp] += pltpu.roll(strength[comp] * weight, offset % count_x, 1)
            for comp in range(3):
                value = sums[comp] + wide(read(ghosts, (3 + comp,), row, 0))
                if row:
                    moved[comp, row : row + 8] = value
                else:
                    moved[comp, 4:8] = value[:4]
                    moved[comp, total_rows - 8 : total_rows - 4] = value[4:]
        for row in range(edge, edge + local_y, 8):
            lateral = [0.0, 0.0, 0.0]
            for offset in range(-2, 3):
                rows = slice(row - offset, row - offset + 8)
                weight = double_weight(offset - TIME_STEP * speeds[now, 1, rows])
                for comp in range(3):
                    lateral[comp] += moved[comp, rows] * weight
            shift = TIME_STEP * speeds[now, 2, row : row + 8]
            rows = slice(row - edge, row - edge + 8)
            for offset in range(-2, 3):
                weight = double_weight(offset - shift)
                slot = (step + 5 + offset) % 5
                for comp in range(3):
                    term = lateral[comp] * weight
                    if offset == -2:
                        out_ref[comp, 0, rows] = total[slot, comp, rows] + term
                    elif offset == 2:
                        total[slot, comp, rows] = term
                    else:
                        total[slot, comp, rows] += term


def remesh(wake, v, v_rims, f, f_rims, ghost, pick):
    _, local_z, local_y, count_x = v.shape
    steps = local_z + 6
    tall = local_y + 16

    def plane(rows, delay, limit):
        return pl.BlockSpec(
            (3, 1, rows, count_x), lambda i, w: (0, jnp.clip(i - delay, 0, limit - 1), 0, 0)
        )

    in_specs = [
        plane(local_y, 3, local_z),
        plane(4, 3, local_z),
        plane(4, 3, local_z),
        plane(local_y + 8, 0, 3),
        plane(local_y + 8, local_z + 3, 3),
        plane(local_y, 4, local_z),
        plane(2, 4, local_z),
        plane(2, 4, local_z),
        plane(local_y + 4, 2, 2),
        plane(local_y + 4, local_z + 4, 2),
        pl.BlockSpec((1, COLUMNS, tall), lambda i, w: (jnp.clip(i - 2, 0, local_z + 3), 0, 0)),
        pl.BlockSpec(pick.shape, lambda i, w: (0, 0)),
    ]
    return pl.pallas_call(
        remesh_kernel,
        grid_spec=pltpu.PrefetchScalarGridSpec(
            num_scalar_prefetch=1,
            grid=(steps,),
            in_specs=in_specs,
            out_specs=pl.BlockSpec(
                (3, 1, local_y, count_x), lambda i, w: (0, jnp.clip(i - 6, 0, local_z - 1), 0, 0)
            ),
            scratch_shapes=[
                pltpu.VMEM((3, 3, tall, count_x), F32),
                pltpu.VMEM((3, tall, count_x), F32),
                pltpu.VMEM((3, tall, count_x), F32),
                pltpu.VMEM((6, tall, 128), F32),
                pltpu.VMEM((5, 3, local_y, count_x), F32),
            ],
        ),
        out_shape=jax.ShapeDtypeStruct(v.shape, F32),
        compiler_params=pltpu.CompilerParams(
            dimension_semantics=("arbitrary",), vmem_limit_bytes=VMEM_BYTES
        ),
        cost_estimate=pl.CostEstimate(flops=v.size * 150, bytes_accessed=v.size * 12, transcendentals=0),
        name="remesh",
    )(wake, v, *v_rims, f, *f_rims, ghost, pick)


def all_rims(cells, rows, planes):
    low, high = rims(cells, "gy", 2, rows)
    local_z = cells.shape[1]
    ends = []
    for part in (slice(local_z - planes, local_z), slice(0, planes)):
        ends.append(jnp.concatenate([low[:, part], cells[:, part], high[:, part]], 2))
    count = lax.axis_size("gz")
    z_low = lax.ppermute(ends[0], "gz", [(i, (i + 1) % count) for i in range(count)])
    z_high = lax.ppermute(ends[1], "gz", [((i + 1) % count, i) for i in range(count)])
    return low, high, z_low, z_high


def diagonal(value, step_y, step_z):
    size_y, size_z = (lax.axis_size("gy"), lax.axis_size("gz"))
    pairs = []
    for y in range(size_y):
        for z in range(size_z):
            target = (y + step_y) % size_y * size_z + (z + step_z) % size_z
            pairs.append((y * size_z + z, target))
    return lax.ppermute(value, ("gy", "gz"), pairs)


def edge_rims(rows, ends, planes):
    local_z = rows.shape[1]
    first, last = (slice(0, planes), slice(local_z - planes, local_z))
    low = diagonal(rows[:, :, 4:], 1, 0)
    high = diagonal(rows[:, :, :4], -1, 0)
    around = []
    for span, part, step in ((last, ends[:, -planes:], 1), (first, ends[:, :planes], -1)):
        around.append(
            jnp.concatenate(
                [
                    diagonal(rows[:, span, 4:], 1, step),
                    diagonal(part, 0, step),
                    diagonal(rows[:, span, :4], -1, step),
                ],
                2,
            )
        )
    return low, high, around[0], around[1]


def ghost_columns(field_planes, thin):
    inner = thin[:, :, 1:-1, 1:-1]
    grad_z = (thin[:, 1:3, 2:, 1:-1] - thin[:, 1:3, :-2, 1:-1]) * 0.5
    grad_y = (thin[:, 1:3, 1:-1, 2:] - thin[:, 1:3, 1:-1, :-2]) * 0.5
    grad_x = (inner[:, 2:4] - inner[:, 0:2]) * 0.5
    pulled = field_planes[0:1] * grad_x + field_planes[1:2] * grad_y + field_planes[2:3] * grad_z
    strength = field_planes + TIME_STEP * pulled
    shift = TIME_STEP * inner[0, 1:3]
    zero = strength[:, 0] * kernel_weight(2.0 - shift[0]) + strength[:, 1] * kernel_weight(1.0 - shift[1])
    one = strength[:, 1] * kernel_weight(2.0 - shift[1])
    columns = jnp.concatenate([inner[:, 2], zero, one], 0)
    columns = jnp.pad(columns, ((0, COLUMNS - columns.shape[0]), (0, 0), (6, 6)))
    return columns.transpose(1, 0, 2)


def body(vorticity, wind):
    field = vorticity[0]
    drift = wind[0]
    count_x = field.shape[3]
    half_x = count_x // 2
    size_gy = lax.axis_size("gy")
    size_gz = lax.axis_size("gz")
    owners = size_gy * size_gz
    local_z, local_y = field.shape[1:3]
    count_y = local_y * size_gy
    count_z = local_z * size_gz
    share = half_x // owners
    chunks = math.gcd(share, 2)
    part = share // chunks
    sizes = (size_gy, size_gz, count_x)
    wake = lax.axis_index("grp").astype(jnp.int32).reshape(1)
    owner = lax.axis_index("gy") * size_gz + lax.axis_index("gz")

    cosine_x, sine_x = angles(count_x)
    alternate = 1.0 - 2.0 * (np.arange(count_x) % 2)
    forward_cos = cosine_x[:, :half_x]
    forward_sin = np.concatenate([alternate[:, None], -sine_x[:, 1:half_x]], 1)
    back_cos = np.concatenate([cosine_x[:1], 2.0 * cosine_x[1:half_x]], 0) / count_x
    back_sin = np.concatenate([-alternate[None, :], 2.0 * sine_x[1:half_x]], 0) / -count_x

    table_y = complex_table(count_y, False)
    table_y = table_y.reshape(2, size_gy, local_y, 2 * count_y)
    table_y = table_y.transpose(1, 0, 2, 3).reshape(2 * count_y, 2 * count_y)
    back_y = complex_table(count_y, True)
    back_y = back_y.reshape(2 * count_y, 2, size_gy, local_y)
    back_y = back_y.transpose(0, 2, 1, 3).reshape(2 * count_y, 2 * count_y)
    cosine_z, sine_z = angles(count_z)
    tables = [jnp.asarray(h) for t in (cosine_z, sine_z, table_y, back_y) for h in halves(t)]

    def dot(letters, values, table):
        return jnp.einsum(letters, values, jnp.asarray(table, F32), precision=HIGH)

    pieces = []
    for chunk in range(chunks):
        def pick(table):
            return table.reshape(count_x, owners, chunks, part)[:, :, chunk].reshape(count_x, -1)

        lines = jnp.concatenate(
            [
                dot("czyx,xk->kczy", field, pick(forward_cos)),
                dot("czyx,xk->kczy", field, pick(forward_sin)),
            ],
            3,
        )
        pieces.append(lax.all_to_all(lines, ("gy", "gz"), split_axis=0, concat_axis=0, tiled=True))

    field_rims = all_rims(field, 2, 2)
    field_planes = rimmed(last_planes(field), (("gy", 3), ("gz", 2)), 2)

    parts = []
    for chunk in range(chunks):
        base = (owner * share + chunk * part).astype(jnp.int32).reshape(1)
        lines = pieces[chunk].reshape(owners, part, 3, local_z, 2 * local_y)
        lines = middle(lines, base, tables, sizes, 1 if chunk == 0 else 0)
        lines = lines.reshape(owners * part, 3, local_z, 2 * local_y)
        parts.append(lax.all_to_all(lines, ("gy", "gz"), split_axis=0, concat_axis=0, tiled=True))

    def turned(table):
        return table.reshape(owners, chunks, part, -1).transpose(1, 0, 2, 3).reshape(half_x, -1)

    back = np.concatenate([turned(back_cos), turned(back_sin)], 0)
    thin = np.zeros((2, 8, half_x))
    thin[:, :4] = back.reshape(2, half_x, count_x)[..., [count_x - 3, count_x - 2, count_x - 1, 0]].transpose(0, 2, 1)
    speed_table, thin_table = [
        [jnp.asarray(h) for h in halves(t)] for t in (back, thin.reshape(16, half_x))
    ]
    velocity, (rows, ends, thin) = speed(parts, drift, speed_table, thin_table)

    velocity_rims = edge_rims(rows, ends, 3)
    thin = thin.reshape(3, 8, local_z, local_y)[:, :4]
    thin = rimmed(thin, (("gy", 3), ("gz", 2)), 3)
    ghost = shifted(ghost_columns(field_planes, thin), "grp", 1)
    choose = np.zeros((COLUMNS, 6, 128), np.float32)
    for comp in range(3):
        choose[comp, comp, 0] = 1.0
        choose[3 + comp, 3 + comp, 0] = 0.25
        choose[6 + comp, 3 + comp, 1] = 0.25
    choose = jnp.asarray(choose.reshape(COLUMNS, 6 * 128))
    result = remesh(wake, velocity, velocity_rims, field, field_rims, ghost, choose)
    return (result[None], velocity[None])


def solution(mesh):
    return jax.shard_map(
        body,
        mesh=mesh,
        in_specs=(P("grp", None, "gz", "gy", None), P("grp", None)),
        out_specs=(P("grp", None, "gz", "gy", None), P("grp", None, "gz", "gy", None)),
        check_vma=False,
    )
```

```python
import functools
import math

import jax
import jax.numpy as jnp
import numpy as np
from jax import lax
from jax.experimental import pallas as pl
from jax.experimental.pallas import tpu as pltpu
from jax.sharding import PartitionSpec as P

TIME_STEP = 0.4
HIGH = lax.Precision.HIGH
BF16 = jnp.bfloat16
F32 = jnp.float32
VMEM_BYTES = 56 * 1024 * 1024
COLUMNS = 16


def shifted(value, axis, steps):
    count = lax.axis_size(axis)
    initial, last = (max(0, -steps), min(count, count - steps))
    return lax.ppermute(value, axis, [(source, source + steps) for source in range(initial, last)])


def rims(cells, axis, dim, width):
    count = lax.axis_size(axis)
    head = lax.slice_in_dim(cells, 0, width, axis=dim)
    tail = lax.slice_in_dim(cells, cells.shape[dim] - width, cells.shape[dim], axis=dim)
    low = lax.ppermute(tail, axis, [(i, (i + 1) % count) for i in range(count)])
    high = lax.ppermute(head, axis, [((i + 1) % count, i) for i in range(count)])
    return low, high


def rimmed(cells, sides, width):
    for axis, dim in sides:
        low, high = rims(cells, axis, dim, width)
        cells = jnp.concatenate([low, cells, high], axis=dim)
    return cells


def kernel_weight(offset):
    mag = jnp.abs(offset)
    inner = 1.0 - 2.5 * mag * mag + 1.5 * mag * mag * mag
    outer = 0.5 * (2.0 - mag) * (2.0 - mag) * (1.0 - mag)
    return jnp.where(mag < 1.0, inner, jnp.where(mag < 2.0, outer, 0.0 * mag))


def double_weight(offset):
    e = jnp.maximum(1.0 - jnp.abs(offset), -1.0)
    u = 1.0 + e
    p = jnp.maximum(e, 0.0)
    return u * u * e + p * p * (2.0 - 4.0 * p)


def angles(count):
    positions = np.arange(count)
    product = positions[:, None] * positions[None, :] % count
    angle = product * (2.0 * np.pi / count)
    return (np.cos(angle), np.sin(angle))


def complex_table(count, inverse):
    cosine, sine = angles(count)
    if inverse:
        cosine, sine = (cosine / count, -sine / count)
    rows_real = np.stack([cosine, -sine], 1)
    rows_imag = np.stack([sine, cosine], 1)
    return np.stack([rows_real, rows_imag], 0)


def halves(table):
    table = np.asarray(table, np.float32)
    high = np.asarray(table, BF16)
    low = np.asarray(table - high.astype(np.float32), BF16)
    return high, low


def split(value):
    high = value.astype(BF16)
    return high, (value - high.astype(F32)).astype(BF16)


def product(left, right, dims=(((1,), (0,)), ((), ()))):
    def one(a, b):
        return lax.dot_general(a, b, dims, preferred_element_type=F32)

    return one(left[0], right[0]) + (one(left[0], right[1]) + one(left[1], right[0]))


def wave(index, count, odd):
    signed = jnp.where(index < count // 2, index, index - count)
    if odd:
        signed = jnp.where(index == count // 2, 0, signed)
    return signed.astype(F32) * (2.0 * math.pi / count)


def middle_kernel(
    sizes, extra, base_ref, lines_ref, cos_h, cos_l, sin_h, sin_l, fwd_h, fwd_l, back_h, back_l, out_ref, spec, keep
):
    size_gy, size_gz, count_x = sizes
    local_z = lines_ref.shape[3]
    width = lines_ref.shape[4]
    count_z = local_z * size_gz
    count_y = spec.shape[2]
    step = pl.program_id(0)
    index_x = base_ref[0] + jnp.maximum(step - extra, 0)
    packed = index_x == 0
    top = jnp.logical_and(packed, step < extra)
    lane = lax.broadcasted_iota(jnp.int32, (count_z, size_gy * width), 1)
    is_real = (lane % width) < width // 2

    def plane():
        def forward(comp, carry):
            rows = []
            for y in range(size_gy):
                parts = [lines_ref[y * size_gz + z, 0, comp] for z in range(size_gz)]
                rows.append(jnp.concatenate(parts, 0))
            if extra:
                moved = [jnp.where(top, pltpu.roll(row, width // 2, 1), row) for row in rows]
                value = jnp.concatenate(moved, 1)
                value = jnp.where(jnp.logical_and(packed, jnp.logical_not(is_real)), 0.0, value)
            else:
                value = jnp.concatenate(rows, 1)
            value = product(split(value), (fwd_h[...], fwd_l[...]))
            real, imag = (split(value[:, :count_y]), split(value[:, count_y:]))
            cosine = (cos_h[...], cos_l[...])
            sine = (sin_h[...], sin_l[...])
            spec[comp] = product(cosine, real) + product(sine, imag)
            spec[3 + comp] = product(cosine, imag) - product(sine, real)
            return carry

        lax.fori_loop(0, 3, forward, 0)
        wave_x = wave(jnp.full((1, 1), index_x, jnp.int32), count_x, False)
        wave_x = jnp.where(top, math.pi, wave_x)
        curl_x = jnp.where(packed, 0.0, wave_x)
        tall = 64
        for first in range(0, count_z, tall):
            rows = pl.ds(first, tall)
            index_z = first + lax.broadcasted_iota(jnp.int32, (tall, 1), 0)
            index_y = lax.broadcasted_iota(jnp.int32, (1, count_y), 1)
            wave_z, wave_y = (wave(index_z, count_z, False), wave(index_y, count_y, False))
            curl_z, curl_y = (wave(index_z, count_z, True), wave(index_y, count_y, True))
            squared = wave_x * wave_x + wave_y * wave_y + wave_z * wave_z
            inverse = jnp.where(squared > 0, 1.0 / jnp.where(squared > 0, squared, 1.0), 0.0)
            inverse = inverse * (1.0 / count_z)
            for part, sign in ((3, -1.0), (0, 1.0)):
                scaled = inverse * sign
                s0, s1, s2 = [spec[part + comp, rows, :] * scaled for comp in range(3)]
                values = (curl_y * s2 - curl_z * s1, curl_z * s0 - curl_x * s2, curl_x * s1 - curl_y * s0)
                for comp in range(3):
                    spec[6 + (3 - part) + comp, rows, :] = values[comp]

        def backward(comp, carry):
            real, imag = (split(spec[6 + comp]), split(spec[9 + comp]))
            cosine = (cos_h[...], cos_l[...])
            sine = (sin_h[...], sin_l[...])
            value = jnp.concatenate(
                [
                    product(cosine, real) - product(sine, imag),
                    product(cosine, imag) + product(sine, real),
                ],
                1,
            )
            value = product(split(value), (back_h[...], back_l[...]))
            if extra:
                for y in range(size_gy):
                    cut = value[:, y * width : (y + 1) * width]

                    @pl.when(top)
                    def _():
                        keep[comp, :, y * width : (y + 1) * width] = pltpu.roll(cut, width // 2, 1)

                saved = keep[comp]
                merge = jnp.logical_and(packed, jnp.logical_not(is_real))
                value = jnp.where(merge, saved, value)
            for y in range(size_gy):
                for z in range(size_gz):
                    out_ref[y * size_gz + z, 0, comp] = value[
                        z * local_z : (z + 1) * local_z, y * width : (y + 1) * width
                    ]
            return carry

        lax.fori_loop(0, 3, backward, 0)

    if extra:
        pl.when(jnp.logical_or(step >= extra, packed))(plane)
    else:
        plane()


def middle(lines, base, tables, sizes, extra):
    size_gy, size_gz, count_x = sizes
    owners, share, _, local_z, width = lines.shape
    count_z = local_z * size_gz
    count_y = size_gy * width // 2
    shape = (owners, 1, 3, local_z, width)

    def at(step, base_ref):
        return (0, jnp.maximum(step - extra, 0), 0, 0, 0)

    def whole(table):
        return pl.BlockSpec(table.shape, lambda step, base_ref: (0, 0))

    flops = (share + extra) * 3 * 4 * 2 * 3 * count_z * (2 * count_y) ** 2
    return pl.pallas_call(
        functools.partial(middle_kernel, sizes, extra),
        grid_spec=pltpu.PrefetchScalarGridSpec(
            num_scalar_prefetch=1,
            grid=(share + extra,),
            in_specs=[pl.BlockSpec(shape, at)] + [whole(t) for t in tables],
            out_specs=pl.BlockSpec(shape, at),
            scratch_shapes=[
                pltpu.VMEM((12, count_z, count_y), F32),
                pltpu.VMEM((3, count_z, 2 * count_y) if extra else (1, 8, 128), F32),
            ],
        ),
        out_shape=jax.ShapeDtypeStruct(lines.shape, F32),
        compiler_params=pltpu.CompilerParams(
            dimension_semantics=("arbitrary",), vmem_limit_bytes=VMEM_BYTES
        ),
        cost_estimate=pl.CostEstimate(flops=flops, bytes_accessed=lines.size * 8, transcendentals=0),
        name="middle",
    )(base, lines, *tables)


def planes_kernel(choose_ref, field_ref, out_ref):
    _, tall, local_y, width = field_ref.shape
    rows = field_ref[0].reshape(tall * local_y, width)
    out_ref[0] = lax.dot_general(
        choose_ref[...], rows, (((1,), (1,)), ((), ())),
        preferred_element_type=F32, precision=lax.Precision.HIGHEST,
    )


def last_planes(field):
    _, local_z, local_y, count_x = field.shape
    tall = 8
    choose = np.zeros((8, 128), np.float32)
    choose[0, 126] = 1.0
    choose[1, 127] = 1.0
    planes = pl.pallas_call(
        planes_kernel,
        grid=(3, local_z // tall),
        in_specs=[
            pl.BlockSpec((8, 128), lambda c, z: (0, 0)),
            pl.BlockSpec((1, tall, local_y, 128), lambda c, z: (c, z, 0, count_x // 128 - 1)),
        ],
        out_specs=pl.BlockSpec((1, 8, tall * local_y), lambda c, z: (c, 0, z)),
        out_shape=jax.ShapeDtypeStruct((3, 8, local_z * local_y), F32),
        compiler_params=pltpu.CompilerParams(dimension_semantics=("arbitrary", "arbitrary")),
        cost_estimate=pl.CostEstimate(flops=field.size * 400, bytes_accessed=field.size * 2, transcendentals=0),
        name="planes",
    )(jnp.asarray(choose), field)
    return planes[:, :2].reshape(3, 2, local_z, local_y)


def block_rows(lines, tall):
    rows = []
    for z in range(tall):
        rows.append(jnp.concatenate([ref[:, 0, z, :] for ref in lines], 0))
    return rows


def speed_kernel(chunks, tall, drift_ref, *refs):
    lines = refs[:chunks]
    table_h, table_l, out_ref = refs[chunks:]
    half = lines[0].shape[3] // 2
    rows = []
    for value in block_rows(lines, tall):
        turned = value.T
        rows.append(jnp.concatenate([turned[:half], turned[half:]], 1))
    left = split(jnp.concatenate(rows, 0))
    value = product(left, (table_h[...], table_l[...])) + drift_ref[pl.program_id(0)]
    out_ref[0] = value.reshape(tall, half, value.shape[1])


def edge_kernel(chunks, tall, drift_ref, *refs):
    lines = refs[:chunks]
    table_h, table_l, thin_h, thin_l, rows_ref, ends_ref, thin_ref = refs[chunks:]
    half = lines[0].shape[3] // 2
    drift = drift_ref[pl.program_id(0)]
    step = pl.program_id(1)
    blocks = block_rows(lines, tall)
    turned = [value.T for value in blocks]
    thin = (thin_h[...], thin_l[...])
    flat = []
    for value in blocks:
        both = product(thin, split(value))
        flat.append(both[:8, :half] + both[8:, half:])
    thin_ref[0] = jnp.concatenate(flat, 1) + drift
    table = (table_h[...], table_l[...])
    rows = []
    for value in turned:
        real = jnp.concatenate([value[:4], value[half - 4 : half]], 0)
        imag = jnp.concatenate([value[half : half + 4], value[2 * half - 4 :]], 0)
        rows.append(jnp.concatenate([real, imag], 1))
    value = product(split(jnp.concatenate(rows, 0)), table) + drift
    rows_ref[0] = value.reshape(tall, 8, value.shape[1])

    @pl.when(jnp.logical_or(step == 0, step == pl.num_programs(1) - 1))
    def _():
        whole = [jnp.concatenate([value[:half], value[half:]], 1) for value in turned]
        ends = product(split(jnp.concatenate(whole, 0)), table) + drift
        ends_ref[0] = ends.reshape(tall, half, ends.shape[1])


def speed(parts, drift, table, thin):
    chunks = len(parts)
    depth, _, local_z, width = parts[0].shape
    count_x = table[0].shape[1]
    half = width // 2
    tall = 8
    steps = local_z // tall
    params = pltpu.CompilerParams(
        dimension_semantics=("arbitrary", "arbitrary"), vmem_limit_bytes=VMEM_BYTES
    )
    line_specs = [pl.BlockSpec((depth, 1, tall, width), lambda c, z, d: (0, c, z, 0))] * chunks

    def whole(tables):
        return [pl.BlockSpec(t.shape, lambda c, z, d: (0, 0)) for t in tables]

    ends = min(2, steps)
    edges = pl.pallas_call(
        functools.partial(edge_kernel, chunks, tall),
        grid_spec=pltpu.PrefetchScalarGridSpec(
            num_scalar_prefetch=1,
            grid=(3, steps),
            in_specs=line_specs + whole(table) + whole(thin),
            out_specs=[
                pl.BlockSpec((1, tall, 8, count_x), lambda c, z, d: (c, z, 0, 0)),
                pl.BlockSpec((1, tall, half, count_x), lambda c, z, d: (c, (z + 1) // steps * (ends - 1), 0, 0)),
                pl.BlockSpec((1, 8, tall * half), lambda c, z, d: (c, 0, z)),
            ],
        ),
        out_shape=[
            jax.ShapeDtypeStruct((3, local_z, 8, count_x), F32),
            jax.ShapeDtypeStruct((3, ends * tall, half, count_x), F32),
            jax.ShapeDtypeStruct((3, 8, local_z * half), F32),
        ],
        compiler_params=params,
        cost_estimate=pl.CostEstimate(
            flops=3 * local_z * half * count_x * 800, bytes_accessed=16 * local_z * half * count_x, transcendentals=0
        ),
        name="edges",
    )(drift, *parts, *table, *thin)
    velocity = pl.pallas_call(
        functools.partial(speed_kernel, chunks, tall),
        grid_spec=pltpu.PrefetchScalarGridSpec(
            num_scalar_prefetch=1,
            grid=(3, steps),
            in_specs=line_specs + whole(table),
            out_specs=pl.BlockSpec((1, tall, half, count_x), lambda c, z, d: (c, z, 0, 0)),
        ),
        out_shape=jax.ShapeDtypeStruct((3, local_z, half, count_x), F32),
        compiler_params=params,
        cost_estimate=pl.CostEstimate(
            flops=3 * local_z * half * count_x * 8000, bytes_accessed=24 * local_z * half * count_x, transcendentals=0
        ),
        name="speed",
    )(drift, *parts, *table)
    return velocity, edges


def remesh_kernel(
    wake_ref, v_ref, vl_ref, vh_ref, vzl_ref, vzh_ref, f_ref, fl_ref, fh_ref, fzl_ref, fzh_ref,
    ghost_ref, pick_ref, out_ref, speeds, field, moved, ghosts, total,
):
    local_y, count_x = v_ref.shape[2:]
    step = pl.program_id(0)
    local_z = pl.num_programs(0) - 6
    wake = wake_ref[0] == 1
    inner = local_y // 8
    here = step % 3

    def blocked(value):
        return value.reshape(value.shape[0], -1, 8, value.shape[-1])

    @pl.when(step == 0)
    def _():
        speeds[...] = jnp.zeros_like(speeds)
        field[...] = jnp.zeros_like(field)
        moved[...] = jnp.zeros_like(moved)
        total[...] = jnp.zeros_like(total)

    def load_speeds(low, middle, high):
        speeds[here, :, 0, 4:8] = low
        speeds[here, :, 1 : inner + 1] = blocked(middle)
        speeds[here, :, inner + 1, 0:4] = high

    def load_field(low, middle, high):
        field[:, 0, 6:8] = low
        field[:, 1 : inner + 1] = blocked(middle)
        field[:, inner + 1, 0:2] = high

    def thirds(ref, width):
        edge = width + local_y
        return ref[:, 0, :width], ref[:, 0, width:edge], ref[:, 0, edge:]

    @pl.when(step < 3)
    def _():
        load_speeds(*thirds(vzl_ref, 4))

    @pl.when(step >= local_z + 3)
    def _():
        load_speeds(*thirds(vzh_ref, 4))

    @pl.when(jnp.logical_and(step >= 3, step < local_z + 3))
    def _():
        load_speeds(vl_ref[:, 0], v_ref[:, 0], vh_ref[:, 0])

    @pl.when(step < 4)
    def _():
        load_field(*thirds(fzl_ref, 2))

    @pl.when(step >= local_z + 4)
    def _():
        load_field(*thirds(fzh_ref, 2))

    @pl.when(jnp.logical_and(step >= 4, step < local_z + 4))
    def _():
        load_field(fl_ref[:, 0], f_ref[:, 0], fh_ref[:, 0])

    @pl.when(step >= 2)
    def _():
        now, before = ((step + 2) % 3, (step + 1) % 3)
        picked = lax.dot_general(
            ghost_ref[0], pick_ref[...], (((0,), (0,)), ((), ())),
            preferred_element_type=F32, precision=lax.Precision.HIGHEST,
        )
        ghosts[...] = picked.reshape(inner + 2, 8, 128)
        lane = lax.broadcasted_iota(jnp.int32, (8, count_x), 1)
        first = jnp.logical_and(lane == 0, wake)
        last = jnp.logical_and(lane == count_x - 1, wake)
        cut = {
            offset: jnp.logical_and(lane >= count_x - offset if offset > 0 else lane < -offset, wake)
            for offset in (-2, -1, 1, 2)
        }

        def wide(value):
            return jnp.concatenate([value, jnp.zeros((8, count_x - 128), F32)], 1)

        row = lax.broadcasted_iota(jnp.int32, (8, count_x), 0)

        def moved_rows(lower, middle, upper, offset):
            if offset == 0:
                return middle
            if offset > 0:
                return pltpu.roll(jnp.where(row >= 8 - offset, lower, middle), offset, 0)
            return pltpu.roll(jnp.where(row < -offset, upper, middle), 8 + offset, 0)

        def ends(ref, *index):
            return jnp.concatenate([ref[(*index, 0)][4:], ref[(*index, inner + 1)][:4]], 0)

        def advanced(vel, below, above, away, vor, ghost):
            small = lax.broadcasted_iota(jnp.int32, (8, 128), 1) < 2
            ghost_v = [pltpu.roll(ghost, -comp % 128, 1) if comp else ghost for comp in range(3)]
            ghost_q = [jnp.where(small, pltpu.roll(ghost, -(4 + 2 * comp) % 128, 1), 0.0) for comp in range(3)]
            vor = [value * 0.125 for value in vor]
            strength = []
            for comp in range(3):
                v = vel[comp]
                left = jnp.where(first, wide(ghost_v[comp]), pltpu.roll(v, 1, 1))
                right = jnp.where(last, v, pltpu.roll(v, count_x - 1, 1))
                pulled = vor[0] * (right - left) + vor[1] * (above[comp] - below[comp]) + vor[2] * away[comp]
                strength.append(vor[comp] + (0.5 * TIME_STEP) * pulled)
            shift = TIME_STEP * vel[0]
            weight = double_weight(-shift)
            sums = [strength[comp] * weight + wide(ghost_q[comp]) for comp in range(3)]
            for offset in (-2, -1, 1, 2):
                weight = jnp.where(cut[offset], 0.0, double_weight(offset - shift))
                for comp in range(3):
                    sums[comp] += pltpu.roll(strength[comp] * weight, offset % count_x, 1)
            return sums

        outer = []
        for comp in range(3):
            low = jnp.concatenate([speeds[now, comp, 0], speeds[now, comp, 1]], 0)
            high = jnp.concatenate([speeds[now, comp, inner], speeds[now, comp, inner + 1]], 0)
            below = jnp.concatenate([low[3:7], high[7:11]], 0)
            above = jnp.concatenate([low[5:9], high[9:13]], 0)
            outer.append((below, above))
        sums = advanced(
            [ends(speeds, now, comp) for comp in range(3)],
            [pair[0] for pair in outer],
            [pair[1] for pair in outer],
            [ends(speeds, here, comp) - ends(speeds, before, comp) for comp in range(3)],
            [ends(field, comp) for comp in range(3)],
            jnp.concatenate([ghosts[0, 4:8], ghosts[inner + 1, 0:4]], 0),
        )
        for comp in range(3):
            moved[comp, 0, 4:8] = sums[comp][:4]
            moved[comp, inner + 1, 0:4] = sums[comp][4:]

        def stretch(block):
            vel = [speeds[now, comp, block] for comp in range(3)]
            lower = [speeds[now, comp, block - 1] for comp in range(3)]
            upper = [speeds[now, comp, block + 1] for comp in range(3)]
            below = [moved_rows(lower[comp], vel[comp], None, 1) for comp in range(3)]
            above = [moved_rows(None, vel[comp], upper[comp], -1) for comp in range(3)]
            sums = advanced(
                vel,
                below,
                above,
                [speeds[here, comp, block] - speeds[before, comp, block] for comp in range(3)],
                [field[comp, block] for comp in range(3)],
                ghosts[block],
            )
            for comp in range(3):
                moved[comp, block] = sums[comp]


        def spread(block):
            around = [[moved[comp, block + away] for away in (-1, 0, 1)] for comp in range(3)]
            along = [TIME_STEP * speeds[now, 1, block + away] for away in (-1, 0, 1)]
            lateral = [0.0, 0.0, 0.0]
            for offset in (0, 1, -1, 2, -2):
                weight = double_weight(offset - moved_rows(*along, offset))
                for comp in range(3):
                    lateral[comp] += moved_rows(*around[comp], offset) * weight
            shift = TIME_STEP * speeds[now, 2, block]
            rows = slice(block * 8 - 8, block * 8)
            for offset in range(-2, 3):
                weight = double_weight(offset - shift)
                slot = (step + 5 + offset) % 5
                for comp in range(3):
                    term = lateral[comp] * weight
                    if offset == -2:
                        out_ref[comp, 0, rows] = total[slot, comp, block - 1] + term
                    elif offset == 2:
                        total[slot, comp, block - 1] = term
                    else:
                        total[slot, comp, block - 1] += term

        for block in range(1, inner + 1):
            stretch(block)
            if block > 1:
                spread(block - 1)
        spread(inner)


def remesh(wake, v, v_rims, f, f_rims, ghost, pick):
    _, local_z, local_y, count_x = v.shape
    steps = local_z + 6
    tall = local_y + 16

    def plane(rows, delay, limit):
        return pl.BlockSpec(
            (3, 1, rows, count_x), lambda i, w: (0, jnp.clip(i - delay, 0, limit - 1), 0, 0)
        )

    in_specs = [
        plane(local_y, 3, local_z),
        plane(4, 3, local_z),
        plane(4, 3, local_z),
        plane(local_y + 8, 0, 3),
        plane(local_y + 8, local_z + 3, 3),
        plane(local_y, 4, local_z),
        plane(2, 4, local_z),
        plane(2, 4, local_z),
        plane(local_y + 4, 2, 2),
        plane(local_y + 4, local_z + 4, 2),
        pl.BlockSpec((1, COLUMNS, tall), lambda i, w: (jnp.clip(i - 2, 0, local_z + 3), 0, 0)),
        pl.BlockSpec(pick.shape, lambda i, w: (0, 0)),
    ]
    return pl.pallas_call(
        remesh_kernel,
        grid_spec=pltpu.PrefetchScalarGridSpec(
            num_scalar_prefetch=1,
            grid=(steps,),
            in_specs=in_specs,
            out_specs=pl.BlockSpec(
                (3, 1, local_y, count_x), lambda i, w: (0, jnp.clip(i - 6, 0, local_z - 1), 0, 0)
            ),
            scratch_shapes=[
                pltpu.VMEM((3, 3, tall // 8, 8, count_x), F32),
                pltpu.VMEM((3, tall // 8, 8, count_x), F32),
                pltpu.VMEM((3, tall // 8, 8, count_x), F32),
                pltpu.VMEM((tall // 8, 8, 128), F32),
                pltpu.VMEM((5, 3, local_y // 8, 8, count_x), F32),
            ],
        ),
        out_shape=jax.ShapeDtypeStruct(v.shape, F32),
        compiler_params=pltpu.CompilerParams(
            dimension_semantics=("arbitrary",), vmem_limit_bytes=VMEM_BYTES
        ),
        cost_estimate=pl.CostEstimate(flops=v.size * 150, bytes_accessed=v.size * 12, transcendentals=0),
        name="remesh",
    )(wake, v, *v_rims, f, *f_rims, ghost, pick)


def diagonal(value, step_y, step_z):
    size_y, size_z = (lax.axis_size("gy"), lax.axis_size("gz"))
    pairs = []
    for y in range(size_y):
        for z in range(size_z):
            target = (y + step_y) % size_y * size_z + (z + step_z) % size_z
            pairs.append((y * size_z + z, target))
    return lax.ppermute(value, ("gy", "gz"), pairs)


def edge_rims(rows, ends, width, planes):
    local_z, count = (rows.shape[1], rows.shape[2])
    first, last = (slice(0, planes), slice(local_z - planes, local_z))
    heads, tails = (slice(0, width), slice(count - width, count))
    low = diagonal(rows[:, :, tails], 1, 0)
    high = diagonal(rows[:, :, heads], -1, 0)
    around = []
    for span, part, step in ((last, ends[:, -planes:], 1), (first, ends[:, :planes], -1)):
        around.append(
            jnp.concatenate(
                [
                    diagonal(rows[:, span, tails], 1, step),
                    diagonal(part, 0, step),
                    diagonal(rows[:, span, heads], -1, step),
                ],
                2,
            )
        )
    return low, high, around[0], around[1]


def surrounded(cells, width):
    local_z, local_y = cells.shape[2:]
    spans = {1: lambda n: slice(n - width, n), 0: lambda n: slice(0, n), -1: lambda n: slice(0, width)}
    lines = []
    for step_z in (1, 0, -1):
        line = []
        for step_y in (1, 0, -1):
            piece = cells[:, :, spans[step_z](local_z), spans[step_y](local_y)]
            line.append(diagonal(piece, step_y, step_z) if step_y or step_z else piece)
        lines.append(jnp.concatenate(line, 3))
    return jnp.concatenate(lines, 2)


def ghost_columns(field_planes, thin):
    inner = thin[:, :, 1:-1, 1:-1]
    grad_z = (thin[:, 1:3, 2:, 1:-1] - thin[:, 1:3, :-2, 1:-1]) * 0.5
    grad_y = (thin[:, 1:3, 1:-1, 2:] - thin[:, 1:3, 1:-1, :-2]) * 0.5
    grad_x = (inner[:, 2:4] - inner[:, 0:2]) * 0.5
    pulled = field_planes[0:1] * grad_x + field_planes[1:2] * grad_y + field_planes[2:3] * grad_z
    strength = field_planes + TIME_STEP * pulled
    shift = TIME_STEP * inner[0, 1:3]
    zero = strength[:, 0] * kernel_weight(2.0 - shift[0]) + strength[:, 1] * kernel_weight(1.0 - shift[1])
    one = strength[:, 1] * kernel_weight(2.0 - shift[1])
    columns = jnp.concatenate([inner[:, 2], zero, one], 0)
    columns = jnp.pad(columns, ((0, COLUMNS - columns.shape[0]), (0, 0), (6, 6)))
    return columns.transpose(1, 0, 2)


def body(vorticity, wind):
    field = vorticity[0]
    drift = wind[0]
    count_x = field.shape[3]
    half_x = count_x // 2
    size_gy = lax.axis_size("gy")
    size_gz = lax.axis_size("gz")
    owners = size_gy * size_gz
    local_z, local_y = field.shape[1:3]
    count_y = local_y * size_gy
    count_z = local_z * size_gz
    share = half_x // owners
    chunks = math.gcd(share, 2)
    part = share // chunks
    sizes = (size_gy, size_gz, count_x)
    wake = lax.axis_index("grp").astype(jnp.int32).reshape(1)
    owner = lax.axis_index("gy") * size_gz + lax.axis_index("gz")

    cosine_x, sine_x = angles(count_x)
    alternate = 1.0 - 2.0 * (np.arange(count_x) % 2)
    forward_cos = cosine_x[:, :half_x]
    forward_sin = np.concatenate([alternate[:, None], -sine_x[:, 1:half_x]], 1)
    back_cos = np.concatenate([cosine_x[:1], 2.0 * cosine_x[1:half_x]], 0) / count_x
    back_sin = np.concatenate([-alternate[None, :], 2.0 * sine_x[1:half_x]], 0) / -count_x

    table_y = complex_table(count_y, False)
    table_y = table_y.reshape(2, size_gy, local_y, 2 * count_y)
    table_y = table_y.transpose(1, 0, 2, 3).reshape(2 * count_y, 2 * count_y)
    back_y = complex_table(count_y, True)
    back_y = back_y.reshape(2 * count_y, 2, size_gy, local_y)
    back_y = back_y.transpose(0, 2, 1, 3).reshape(2 * count_y, 2 * count_y)
    cosine_z, sine_z = angles(count_z)
    tables = [jnp.asarray(h) for t in (cosine_z, sine_z, table_y, back_y) for h in halves(t)]

    def dot(letters, values, table):
        return jnp.einsum(letters, values, jnp.asarray(table, F32), precision=HIGH)

    def pick(table, chunk):
        return table.reshape(count_x, owners, chunks, part)[:, :, chunk].reshape(count_x, -1)

    field_rims = edge_rims(field, field, 2, 2)
    field_planes = surrounded(last_planes(field), 2)
    pieces = []
    for chunk in range(chunks):
        lines = jnp.concatenate(
            [
                dot("czyx,xk->kczy", field, pick(forward_cos, chunk)),
                dot("czyx,xk->kczy", field, pick(forward_sin, chunk)),
            ],
            3,
        )
        pieces.append(lax.all_to_all(lines, ("gy", "gz"), split_axis=0, concat_axis=0, tiled=True))

    parts = []
    for chunk in range(chunks):
        base = (owner * share + chunk * part).astype(jnp.int32).reshape(1)
        lines = pieces[chunk].reshape(owners, part, 3, local_z, 2 * local_y)
        lines = middle(lines, base, tables, sizes, 1 if chunk == 0 else 0)
        lines = lines.reshape(owners * part, 3, local_z, 2 * local_y)
        parts.append(lax.all_to_all(lines, ("gy", "gz"), split_axis=0, concat_axis=0, tiled=True))

    def turned(table):
        return table.reshape(owners, chunks, part, -1).transpose(1, 0, 2, 3).reshape(half_x, -1)

    back = np.concatenate([turned(back_cos), turned(back_sin)], 0)
    thin = np.zeros((2, 8, half_x))
    thin[:, :4] = back.reshape(2, half_x, count_x)[..., [count_x - 3, count_x - 2, count_x - 1, 0]].transpose(0, 2, 1)
    speed_table, thin_table = [
        [jnp.asarray(h) for h in halves(t)] for t in (back, thin.reshape(16, half_x))
    ]
    velocity, (rows, ends, thin) = speed(parts, drift, speed_table, thin_table)

    velocity_rims = edge_rims(rows, ends, 4, 3)
    thin = thin.reshape(3, 8, local_z, local_y)[:, :4]
    thin = rimmed(thin, (("gy", 3), ("gz", 2)), 3)
    ghost = shifted(ghost_columns(field_planes, thin), "grp", 1)
    choose = np.zeros((COLUMNS, 128), np.float32)
    for comp in range(3):
        choose[comp, comp] = 1.0
        choose[3 + comp, 4 + 2 * comp] = 0.25
        choose[6 + comp, 5 + 2 * comp] = 0.25
    choose = jnp.asarray(choose)
    result = remesh(wake, velocity, velocity_rims, field, field_rims, ghost, choose)
    return (result[None], velocity[None])


def solution(mesh):
    return jax.shard_map(
        body,
        mesh=mesh,
        in_specs=(P("grp", None, "gz", "gy", None), P("grp", None)),
        out_specs=(P("grp", None, "gz", "gy", None), P("grp", None, "gz", "gy", None)),
        check_vma=False,
    )
```
